32 devices in a mesh: blk: 8 (over y, x, core), org: 4 (over z).
Axes of the slice: x: 2, y: 2, z: 4, core: 2. Of those that a mesh axis runs over, the one named last changes fastest.
Arguments:
- warm_labels: float32 [64, 512, 1024], P('blk', None, 'org'), may hold values from 0 to 6
- link_costs: float32 [4, 64, 512], P(None, 'blk'), may hold values from 0.05 to 1.5
- anchor_nodes: int32 [1024], P('org'), may hold values from 0 to 32767
- demand: float32 [1024], P('org'), may hold values from 0.2 to 2
Outputs:
- labels: float32 [64, 512, 1024], P('blk', None, 'org')
- link_weights: float32 [4, 64, 512], P(None, 'blk', 'org')
The draws below stay inside these ranges and needn't reach their ends.
Inputs may be any that keep to these rules, and one draw needn't show every extreme that they name: `anchor_nodes`: node numbers r * 512 + c.
All inputs are finite; a program needn't handle non-finite values.
Results may differ from the reference program's by a relative error of at most 0.0003.
Values sent between devices are 32-bit elements; how exact they have to be, the bound alone decides.
A program may use at most 128 MiB of HBM per device.

```python
import math
import jax
import jax.numpy as jnp
from jax import lax

ROWS_DEV = 8
GCOLS = 512
ANCHORS = 1024
INNER = 2
ROUNDS = 3
NROWS = 64
NODES = 32768
N_BLK = 8


def place_ends(array, stream_key, smallest, high):
    longest = array.shape.index(max(array.shape))
    spots = []
    for shift in (0, 1):
        where = [jax.random.randint(jax.random.fold_in(stream_key, axis), (), 0, length) for axis, length in enumerate(array.shape)]
        where[longest] = (where[longest] + shift) % array.shape[longest]
        spots.append(tuple(where))
    return array.at[spots[0]].set(smallest).at[spots[1]].set(high)


def block_scale(rng, extent, cuts, smallest, top_value):
    level = 1.0
    for position, blocks in cuts:
        steps = jax.random.uniform(jax.random.fold_in(jax.random.fold_in(rng, 6), position), (blocks,), jnp.float32, smallest / len(cuts), top_value / len(cuts))
        level = level * jnp.repeat(jnp.exp(steps), extent[position] // blocks).reshape((-1,) + (1,) * (len(extent) - 1 - position))
    return level


def setup_inputs(seed: int = 0) -> dict:
    key_list = jax.random.split(jax.random.key(seed), 5)
    warm_labels = jnp.clip(6.0 * jax.random.uniform(key_list[0], (NROWS, GCOLS, ANCHORS), jnp.float32) ** block_scale(key_list[0], (NROWS, GCOLS, ANCHORS), ((0, 8), (2, 4)), -0.2, 0.2), 0.0, 6.0)
    link_costs = jnp.clip(jnp.exp(math.log(1.5) - 3.4011974 * jax.random.uniform(key_list[1], (4, NROWS, GCOLS), jnp.float32) ** block_scale(key_list[1], (4, NROWS, GCOLS), ((1, 8),), -0.2, 0.2)), 0.05, 1.5)
    anchor_nodes = place_ends(jax.random.randint(key_list[2], (ANCHORS,), 0, NODES), jax.random.fold_in(key_list[2], 1), 0, NODES - 1).astype(jnp.int32)
    demand = jnp.clip(jnp.exp(math.log(2.0) - 2.3025851 * jax.random.uniform(key_list[3], (ANCHORS,), jnp.float32) ** block_scale(key_list[3], (ANCHORS,), ((0, 4),), -0.2, 0.2)), 0.2, 2.0)
    return dict(warm_labels=warm_labels, link_costs=link_costs, anchor_nodes=anchor_nodes, demand=demand)


far_value = 1e9
temper = 0.5


def relax_step(padded, costs):
    centre = padded[1:-1]
    edge = jnp.full((centre.shape[0], 1, centre.shape[2]), far_value, centre.dtype)
    west = jnp.concatenate([edge, centre[:, :-1]], axis=1) + costs[0, 1:-1][:, :, None]
    east = jnp.concatenate([centre[:, 1:], edge], axis=1) + costs[1, 1:-1][:, :, None]
    north = padded[:-2] + costs[2, 1:-1][:, :, None]
    south = padded[2:] + costs[3, 1:-1][:, :, None]
    return jnp.minimum(jnp.minimum(jnp.minimum(centre, west), jnp.minimum(east, north)), south)


def link_terms(padded, labels, costs, weights):
    edge = jnp.full((labels.shape[0], 1, labels.shape[2]), far_value, labels.dtype)
    sides = (jnp.concatenate([edge, labels[:, :-1]], axis=1),
             jnp.concatenate([labels[:, 1:], edge], axis=1),
             padded[:-2], padded[2:])
    result = []
    for side in range(4):
        expo = jnp.exp(-temper * (sides[side] + costs[side][:, :, None] - labels))
        result.append(jnp.einsum("rco,o->rc", expo, weights, precision=lax.Precision.HIGHEST))
    return jnp.stack(result)


def reference(warm_labels, link_costs, anchor_nodes, demand):
    total_rows = ROWS_DEV * N_BLK
    node_ids = (jnp.arange(total_rows, dtype=jnp.int32)[:, None] * GCOLS
                + jnp.arange(GCOLS, dtype=jnp.int32)[None, :]).astype(jnp.int32)
    block = 128 if ANCHORS % 128 == 0 else ANCHORS
    blocks = ANCHORS // block
    warm_blocks = warm_labels.reshape(total_rows, GCOLS, blocks, block).transpose(2, 0, 1, 3)
    cost_pad = jnp.pad(link_costs, ((0, 0), (1, 1), (0, 0)))

    def one_block(packed):
        warm, anchors, weights = packed
        labels = jnp.where(node_ids[:, :, None] == anchors[None, None, :], jnp.zeros_like(warm), warm)
        for sweep in range(ROUNDS * INNER):
            padded = jnp.pad(labels, ((1, 1), (0, 0), (0, 0)), constant_values=far_value)
            labels = relax_step(padded, cost_pad)
        padded = jnp.pad(labels, ((1, 1), (0, 0), (0, 0)), constant_values=far_value)
        return labels, link_terms(padded, labels, link_costs, weights)

    label_blocks, partials = lax.map(one_block, (warm_blocks, anchor_nodes.reshape(blocks, block),
                                                 demand.reshape(blocks, block)))
    labels = label_blocks.transpose(1, 2, 0, 3).reshape(total_rows, GCOLS, ANCHORS)
    link_weights = jnp.sum(partials, axis=0) / ANCHORS
    return labels, link_weights
```

```python
import functools

import jax
import jax.numpy as jnp
from jax import lax
from jax.experimental import pallas as pl
from jax.experimental.pallas import tpu as pltpu
from jax.sharding import PartitionSpec as P

INNER = 2
ROUNDS = 3
STEPS = INNER * ROUNDS
HALO = STEPS + 1

far_value = 1000000000.0
temper = 0.5
LANES = 128
PAD = 8
CHUNK = 64
MESH = pl.DeviceIdType.MESH


def kernel(n, m, rows, cols, halves, warm, costs, anchors, demand, out, weights, grid, wide, raw, turned, sums, share,
           landed, row_send, row_recv, cost_send, cost_recv, org_send, org_recv, local_sem, out_sem):
    me = lax.axis_index("blk")
    org = lax.axis_index("org")
    has_top = me > 0
    has_bottom = me < n - 1
    top = {"blk": jnp.maximum(me - 1, 0)}
    bottom = {"blk": jnp.minimum(me + 1, n - 1)}
    first, last = HALO, HALO + rows - 1
    inner = pl.ds(PAD, cols)
    sides = ((has_top, top), (has_bottom, bottom))

    barrier = pltpu.get_barrier_semaphore()
    for there, who in sides:
        @pl.when(there)
        def _():
            pl.semaphore_signal(barrier, inc=1, device_id=who, device_id_type=MESH)
    for d in range(1, m):
        pl.semaphore_signal(barrier, inc=1, device_id={"org": lax.rem(org + d, m)}, device_id_type=MESH)
    own_cost = pltpu.make_async_copy(costs, raw.at[0], local_sem.at[halves])
    own_cost.start()

    def own_rows(h):
        return pltpu.make_async_copy(
            warm.at[:, :, pl.ds(h * LANES, LANES)],
            grid.at[0, h, pl.ds(first, rows), inner, :],
            local_sem.at[h])
    for h in range(halves):
        own_rows(h).start()
    pl.semaphore_wait(barrier, m - 1 + jnp.where(has_top, 1, 0) + jnp.where(has_bottom, 1, 0))

    def cost_copy(side):
        return pltpu.make_async_remote_copy(
            src_ref=costs, dst_ref=raw.at[2 - side], send_sem=cost_send.at[side], recv_sem=cost_recv.at[side],
            device_id=sides[side][1], device_id_type=MESH)

    def row_copy(side, h, j):
        source = j - 1 if side == 0 else rows - j
        target = last + j if side == 0 else first - j
        lanes = pl.ds(pl.multiple_of(h * LANES, LANES), LANES)
        return pltpu.make_async_remote_copy(
            src_ref=warm.at[source, :, lanes], dst_ref=grid.at[0, h, target, inner, :],
            send_sem=row_send.at[side, h, j - 1], recv_sem=row_recv.at[side, h, j - 1],
            device_id=sides[side][1], device_id_type=MESH)

    for side in range(2):
        @pl.when(sides[side][0])
        def _():
            cost_copy(side).start()
    for h in range(halves):
        def send_rows(j, carry):
            for side in range(2):
                @pl.when(sides[side][0])
                def _():
                    row_copy(side, h, j).start()
            return carry
        lax.fori_loop(1, HALO + 1, send_rows, 0)

    edge = jnp.full((PAD, LANES), far_value, jnp.float32)
    total = rows + 2 * HALO

    def fill_edges(r, carry):
        for b in range(2):
            for h in range(halves):
                grid[b, h, r, pl.ds(0, PAD), :] = edge
                grid[b, h, r, pl.ds(PAD + cols, PAD), :] = edge
        return carry
    lax.fori_loop(0, total, fill_edges, 0)
    raw[3] = jnp.zeros_like(raw[3])
    for missing, block, begin in ((me == 0, 1, 0), (me == n - 1, 2, last + 1)):
        @pl.when(missing)
        def _():
            raw[block] = jnp.full(raw.shape[1:], far_value, jnp.float32)
            def fill(r, carry):
                for h in range(halves):
                    grid[0, h, begin + r, inner, :] = jnp.full((cols, LANES), far_value, jnp.float32)
                return carry
            lax.fori_loop(0, HALO, fill, 0)

    own_cost.wait()
    for side in range(2):
        @pl.when(sides[1 - side][0])
        def _():
            cost_copy(side).wait_recv()
    turned[...] = jnp.transpose(raw[...].reshape(4 * 4 * rows, cols))

    def widen(i, carry):
        piece = turned[pl.ds(pl.multiple_of(i * 8, 8), 8), :]
        for r in range(1, total - 1):
            if r < first:
                block, row = 1, rows - first + r
            elif r <= last:
                block, row = 0, r - first
            else:
                block, row = 2, r - last - 1
            for k in range(4):
                lane = (block * 4 + k) * rows + row
                wide[k, r, pl.ds(pl.multiple_of(i * 8, 8), 8), :] = jnp.broadcast_to(piece[:, lane:lane + 1], (8, LANES))
        return carry
    lax.fori_loop(0, cols // 8, widen, 0)

    def place(h, r):
        names = anchors[h]
        base = (me * rows + r - first) * cols
        for i in range(cols // CHUNK):
            node = lax.broadcasted_iota(jnp.int32, (CHUNK, LANES), 0) + (base + i * CHUNK)
            at = pl.ds(PAD + i * CHUNK, CHUNK)
            grid[0, h, r, at, :] = jnp.where(node == names, 0.0, grid[0, h, r, at, :])

    def relax(h, r, s):
        old, new = lax.rem(s + 1, 2), lax.rem(s, 2)
        for i in range(cols // CHUNK):
            c0 = PAD + i * CHUNK
            at, cut = pl.ds(c0, CHUNK), pl.ds(i * CHUNK, CHUNK)
            best = grid[old, h, r, at, :]
            best = jnp.minimum(best, grid[old, h, r, pl.ds(c0 - 1, CHUNK), :] + wide[0, r, cut, :])
            best = jnp.minimum(best, grid[old, h, r, pl.ds(c0 + 1, CHUNK), :] + wide[1, r, cut, :])
            best = jnp.minimum(best, grid[old, h, r - 1, at, :] + wide[2, r, cut, :])
            best = jnp.minimum(best, grid[old, h, r + 1, at, :] + wide[3, r, cut, :])
            grid[new, h, r, at, :] = best

    ones = jnp.ones((8, 2 * LANES), jnp.bfloat16)
    sums[...] = jnp.zeros_like(sums)
    middle = rows // 2
    zero_edge = jnp.zeros((PAD, LANES), jnp.float32)

    def half(h, carry):
        own_rows(h).wait()

        def place_own(r, carry):
            place(h, r)
            return carry
        lax.fori_loop(first, last + 1, place_own, 0)
        for s in range(1, middle):
            def inside(r, carry):
                relax(h, r, jnp.int32(s))
                return carry
            lax.fori_loop(first + s, last - s + 1, inside, 0)

        def stage(j, carry):
            for side in range(2):
                @pl.when(sides[1 - side][0])
                def _():
                    row_copy(side, h, j).wait_recv()
            place(h, first - j)
            place(h, last + j)

            def diagonal(s, carry):
                relax(h, first - j + s, s)
                relax(h, last + j - s, s)
                return carry
            return lax.fori_loop(1, jnp.minimum(STEPS, j + middle - 1) + 1, diagonal, carry)
        lax.fori_loop(1, HALO + 1, stage, 0)
        out_copy(h).start()

        def small(r, carry):
            grid[1, h, r, pl.ds(0, PAD), :] = zero_edge
            grid[1, h, r, pl.ds(PAD + cols, PAD), :] = zero_edge
            for i in range(cols // CHUNK):
                at = pl.ds(PAD + i * CHUNK, CHUNK)
                grid[1, h, r, at, :] = jnp.exp(-temper * grid[0, h, r, at, :])
            return carry
        lax.fori_loop(first - 1, last + 2, small, 0)

        def add_links(q, carry):
            r = first + q
            own = demand[h] * jnp.exp(temper * grid[0, h, r, inner, :])
            places = ((r, PAD - 1), (r, PAD + 1), (r - 1, PAD), (r + 1, PAD))
            for k, (row, start) in enumerate(places):
                term = own * grid[1, h, row, pl.ds(start, cols), :]
                high = term.astype(jnp.bfloat16)
                low = (term - high.astype(jnp.float32)).astype(jnp.bfloat16)
                part = lax.dot_general(ones, jnp.concatenate([high, low], axis=1), (((1,), (1,)), ((), ())),
                                       preferred_element_type=jnp.float32)
                sums[k, pl.ds(q, 1), :] += part[0:1]
            return carry
        lax.fori_loop(0, rows, add_links, 0)
        return carry

    def out_copy(h):
        lanes = pl.ds(pl.multiple_of(h * LANES, LANES), LANES)
        return pltpu.make_async_copy(grid.at[0, h, pl.ds(first, rows), inner, :], out.at[:, :, lanes], out_sem.at[h])

    lax.fori_loop(0, halves, half, 0)

    scale = 1.0 / (m * halves * LANES)
    ours = sums[...] * jnp.exp(-temper * raw[0]) * scale
    width = cols // m
    for p in range(m):
        share[p] = ours[:, :, p * width:(p + 1) * width]

    def org_copy(d):
        peer = lax.rem(org + d, m)
        return pltpu.make_async_remote_copy(
            src_ref=share.at[peer], dst_ref=landed.at[d - 1], send_sem=org_send.at[d - 1], recv_sem=org_recv.at[d - 1],
            device_id={"org": peer}, device_id_type=MESH)
    for d in range(1, m):
        org_copy(d).start()
    final = share[org]
    for d in range(1, m):
        org_copy(d).wait_recv()
        final += landed[d - 1]
    weights[...] = final

    for d in range(1, m):
        org_copy(d).wait_send()
    for h in range(halves):
        out_copy(h).wait()
    for side in range(2):
        @pl.when(sides[side][0])
        def _():
            cost_copy(side).wait_send()
            for h in range(halves):
                def sent(j, carry):
                    row_copy(side, h, j).wait_send()
                    return carry
                lax.fori_loop(1, HALO + 1, sent, 0)


def local(n, m, warm_labels, link_costs, anchor_nodes, demand):
    rows, cols, count = warm_labels.shape
    halves = count // LANES
    total = rows + 2 * HALO
    width = cols // m
    any_space = pl.BlockSpec(memory_space=pl.ANY)
    vmem = pl.BlockSpec(memory_space=pltpu.VMEM)
    dma = pltpu.SemaphoreType.DMA
    return pl.pallas_call(
        functools.partial(kernel, n, m, rows, cols, halves),
        out_shape=(
            jax.ShapeDtypeStruct((rows, cols, count), jnp.float32),
            jax.ShapeDtypeStruct((4, rows, width), jnp.float32),
        ),
        in_specs=[any_space, any_space, vmem, vmem],
        out_specs=(any_space, vmem),
        scratch_shapes=[
            pltpu.VMEM((2, halves, total, cols + 2 * PAD, LANES), jnp.float32),
            pltpu.VMEM((4, total, cols, LANES), jnp.float32),
            pltpu.VMEM((4, 4, rows, cols), jnp.float32),
            pltpu.VMEM((cols, 16 * rows), jnp.float32),
            pltpu.VMEM((4, rows, cols), jnp.float32),
            pltpu.VMEM((m, 4, rows, width), jnp.float32),
            pltpu.VMEM((max(m - 1, 1), 4, rows, width), jnp.float32),
            dma((2, halves, HALO)),
            dma((2, halves, HALO)),
            dma((2,)),
            dma((2,)),
            dma((max(m - 1, 1),)),
            dma((max(m - 1, 1),)),
            dma((halves + 1,)),
            dma((halves,)),
        ],
        compiler_params=pltpu.CompilerParams(collective_id=0, has_side_effects=True, vmem_limit_bytes=60 * 1024 * 1024),
    )(warm_labels, link_costs, anchor_nodes.reshape(halves, 1, LANES), demand.reshape(halves, 1, LANES))


def solution(mesh):
    placed = (P("blk", None, "org"), P(None, "blk", None), P("org"), P("org"))
    return jax.shard_map(
        functools.partial(local, mesh.shape["blk"], mesh.shape["org"]),
        mesh=mesh,
        in_specs=placed,
        out_specs=(P("blk", None, "org"), P(None, "blk", "org")),
        check_vma=False,
    )
```

```python
import functools

import jax
import jax.numpy as jnp
from jax import lax
from jax.experimental import pallas as pl
from jax.experimental.pallas import tpu as pltpu
from jax.sharding import PartitionSpec as P

INNER = 2
ROUNDS = 3
STEPS = INNER * ROUNDS
HALO = STEPS + 1

far_value = 1000000000.0
temper = 0.5
LANES = 128
PAD = 8
CHUNK = 64
MESH = pl.DeviceIdType.MESH
GROUPS = ((1, HALO - 3), (HALO - 2, HALO - 1), (HALO, HALO))


def kernel(n, m, rows, cols, halves, warm, costs, anchors, demand, out, weights, grid, wide, raw, turned, sums, share,
           landed, relay, decay, row_send, row_recv, relay_in, relay_out, cost_send, cost_recv, org_send, org_recv, local_sem, out_sem):
    me = lax.axis_index("blk")
    org = lax.axis_index("org")
    has_top = me > 0
    has_bottom = me < n - 1
    top = {"blk": jnp.maximum(me - 1, 0)}
    bottom = {"blk": jnp.minimum(me + 1, n - 1)}
    first, last = HALO, HALO + rows - 1
    inner = pl.ds(PAD, cols)
    sides = ((has_top, top), (has_bottom, bottom))
    mid = n // 2
    relayed = n == 8
    via = (0, n - 1)
    goal = (mid - 1, mid)
    splits = tuple(relayed and me == goal[1 - side] for side in range(2))
    cut = cols // 2

    barrier = pltpu.get_barrier_semaphore()
    for there, who in sides:
        @pl.when(there)
        def _():
            pl.semaphore_signal(barrier, inc=1, device_id=who, device_id_type=MESH)
    for d in range(1, m):
        pl.semaphore_signal(barrier, inc=1, device_id={"org": lax.rem(org + d, m)}, device_id_type=MESH)
    if relayed:
        for a, b in ((mid - 1, 0), (mid - 1, n - 1), (mid, 0), (mid, n - 1)):
            for mine, other in ((a, b), (b, a)):
                @pl.when(me == mine)
                def _():
                    pl.semaphore_signal(barrier, inc=1, device_id={"blk": other}, device_id_type=MESH)
    own_cost = pltpu.make_async_copy(costs, raw.at[0], local_sem.at[halves])
    own_cost.start()

    def own_rows(h):
        return pltpu.make_async_copy(
            warm.at[:, :, pl.ds(h * LANES, LANES)],
            grid.at[0, h, pl.ds(first, rows), inner, :],
            local_sem.at[h])
    for h in range(halves):
        own_rows(h).start()
    pl.semaphore_wait(barrier, m - 1 + jnp.where(has_top, 1, 0) + jnp.where(has_bottom, 1, 0)
                      + (jnp.where((me == 0) | (me == n - 1) | (me == mid) | (me == mid - 1), 2, 0) if relayed else 0))

    def cost_copy(side):
        return pltpu.make_async_remote_copy(
            src_ref=costs, dst_ref=raw.at[2 - side], send_sem=cost_send.at[side], recv_sem=cost_recv.at[side],
            device_id=sides[side][1], device_id_type=MESH)

    def ranges(side, g):
        low, high = GROUPS[g]
        count = high - low + 1
        if side == 0:
            return pl.ds(low - 1, count), pl.ds(last + low, count), pl.ds(low - 1, count)
        return pl.ds(rows - high, count), pl.ds(first - high, count), pl.ds(first - high, count)

    def lane_range(h):
        return pl.ds(pl.multiple_of(h * LANES, LANES), LANES)

    def row_copy(side, h, g, width):
        source, target, _ = ranges(side, g)
        return pltpu.make_async_remote_copy(
            src_ref=warm.at[source, pl.ds(0, width), lane_range(h)],
            dst_ref=grid.at[0, h, target, pl.ds(PAD, width), :],
            send_sem=row_send.at[side, h, g, 0], recv_sem=row_recv.at[side, h, g, 0],
            device_id=sides[side][1], device_id_type=MESH)

    def to_relay(side, h, g):
        source, _, slots = ranges(side, g)
        return pltpu.make_async_remote_copy(
            src_ref=warm.at[source, pl.ds(cut, cols - cut), lane_range(h)],
            dst_ref=relay.at[h, slots],
            send_sem=row_send.at[side, h, g, 1], recv_sem=relay_in.at[h, g],
            device_id={"blk": via[side]}, device_id_type=MESH)

    def from_relay(side, h, g):
        _, target, slots = ranges(side, g)
        return pltpu.make_async_remote_copy(
            src_ref=relay.at[h, slots],
            dst_ref=grid.at[0, h, target, pl.ds(PAD + cut, cols - cut), :],
            send_sem=relay_out.at[h, g], recv_sem=row_recv.at[side, h, g, 1],
            device_id={"blk": goal[side]}, device_id_type=MESH)

    def each_send(h, g, act):
        for side in range(2):
            there, split = sides[side][0], splits[side]
            @pl.when(there & jnp.logical_not(split) if relayed else there)
            def _():
                act(row_copy(side, h, g, cols))
            if relayed:
                @pl.when(split)
                def _():
                    act(to_relay(side, h, g))
                    act(row_copy(side, h, g, cut))

    def arrive(h, g):
        for side in range(2):
            there, split = sides[1 - side][0], splits[1 - side]
            @pl.when(there & jnp.logical_not(split) if relayed else there)
            def _():
                row_copy(side, h, g, cols).wait_recv()
            if relayed:
                @pl.when(split)
                def _():
                    row_copy(side, h, g, cut).wait_recv()
                    from_relay(side, h, g).wait_recv()

    for side in range(2):
        @pl.when(sides[side][0])
        def _():
            cost_copy(side).start()
    for h in range(halves):
        for g in range(len(GROUPS)):
            each_send(h, g, lambda copy: copy.start())

    edge = jnp.full((PAD, LANES), far_value, jnp.float32)
    total = rows + 2 * HALO

    def fill_edges(r, carry):
        for b in range(2):
            for h in range(halves):
                grid[b, h, r, pl.ds(0, PAD), :] = edge
                grid[b, h, r, pl.ds(PAD + cols, PAD), :] = edge
        return carry
    lax.fori_loop(0, total, fill_edges, 0)
    raw[3] = jnp.zeros_like(raw[3])
    for missing, block, begin in ((me == 0, 1, 0), (me == n - 1, 2, last + 1)):
        @pl.when(missing)
        def _():
            raw[block] = jnp.full(raw.shape[1:], far_value, jnp.float32)
            def fill(r, carry):
                for h in range(halves):
                    grid[0, h, begin + r, inner, :] = jnp.full((cols, LANES), far_value, jnp.float32)
                return carry
            lax.fori_loop(0, HALO, fill, 0)

    own_cost.wait()
    for side in range(2):
        @pl.when(sides[1 - side][0])
        def _():
            cost_copy(side).wait_recv()
    turned[...] = jnp.transpose(raw[...].reshape(4 * 4 * rows, cols))

    def widen(i, carry):
        piece = turned[pl.ds(pl.multiple_of(i * 8, 8), 8), :]
        for r in range(1, total - 1):
            if r < first:
                block, row = 1, rows - first + r
            elif r <= last:
                block, row = 0, r - first
            else:
                block, row = 2, r - last - 1
            for k in range(4):
                lane = (block * 4 + k) * rows + row
                wide[k, r, pl.ds(pl.multiple_of(i * 8, 8), 8), :] = jnp.broadcast_to(piece[:, lane:lane + 1], (8, LANES))
        return carry
    lax.fori_loop(0, cols // 8, widen, 0)

    def place(h, r):
        names = anchors[h]
        base = (me * rows + r - first) * cols
        for i in range(cols // CHUNK):
            node = lax.broadcasted_iota(jnp.int32, (CHUNK, LANES), 0) + (base + i * CHUNK)
            at = pl.ds(PAD + i * CHUNK, CHUNK)
            grid[0, h, r, at, :] = jnp.where(node == names, 0.0, grid[0, h, r, at, :])

    def relax(h, r, s):
        old, new = lax.rem(s + 1, 2), lax.rem(s, 2)
        for i in range(cols // CHUNK):
            c0 = PAD + i * CHUNK
            at, cut = pl.ds(c0, CHUNK), pl.ds(i * CHUNK, CHUNK)
            best = grid[old, h, r, at, :]
            best = jnp.minimum(best, grid[old, h, r, pl.ds(c0 - 1, CHUNK), :] + wide[0, r, cut, :])
            best = jnp.minimum(best, grid[old, h, r, pl.ds(c0 + 1, CHUNK), :] + wide[1, r, cut, :])
            best = jnp.minimum(best, grid[old, h, r - 1, at, :] + wide[2, r, cut, :])
            best = jnp.minimum(best, grid[old, h, r + 1, at, :] + wide[3, r, cut, :])
            grid[new, h, r, at, :] = best

    ones = jnp.ones((8, 2 * LANES), jnp.bfloat16)
    sums[...] = jnp.zeros_like(sums)
    middle = rows // 2
    zero_edge = jnp.zeros((PAD, LANES), jnp.float32)
    for r in range(rows + 2):
        decay[r, pl.ds(0, PAD), :] = zero_edge
        decay[r, pl.ds(PAD + cols, PAD), :] = zero_edge

    def half(h, carry):
        own_rows(h).wait()

        def place_own(r, carry):
            place(h, r)
            return carry
        lax.fori_loop(first, last + 1, place_own, 0)
        for s in range(1, middle):
            def inside(r, carry):
                relax(h, r, jnp.int32(s))
                return carry
            lax.fori_loop(first + s, last - s + 1, inside, 0)

        def stage(j, carry):
            place(h, first - j)
            place(h, last + j)

            def diagonal(s, carry):
                relax(h, first - j + s, s)
                relax(h, last + j - s, s)
                return carry
            return lax.fori_loop(1, jnp.minimum(STEPS, j + middle - 1) + 1, diagonal, carry)

        def small(r, carry):
            for i in range(cols // CHUNK):
                at = pl.ds(PAD + i * CHUNK, CHUNK)
                decay[r - first + 1, at, :] = jnp.exp(-temper * grid[0, h, r, at, :])
            return carry

        def add_link(k, own, r, row, start):
            term = own * decay[row - first + 1, pl.ds(start, cols), :]
            high = term.astype(jnp.bfloat16)
            low = (term - high.astype(jnp.float32)).astype(jnp.bfloat16)
            part = lax.dot_general(ones, jnp.concatenate([high, low], axis=1), (((1,), (1,)), ((), ())),
                                   preferred_element_type=jnp.float32)
            sums[k, pl.ds(r - first, 1), :] += part[0:1]

        def growth(r):
            return demand[h] * jnp.exp(temper * grid[0, h, r, inner, :])

        def along(r, carry):
            own = growth(r)
            add_link(0, own, r, r, PAD - 1)
            add_link(1, own, r, r, PAD + 1)
            return carry

        def across(r, carry):
            add_link(3, growth(r), r, r + 1, PAD)
            add_link(2, growth(r + 1), r + 1, r, PAD)
            return carry

        for g in range(len(GROUPS) - 1):
            arrive(h, g)
            lax.fori_loop(GROUPS[g][0], GROUPS[g][1] + 1, stage, 0)
        out_copy(h).start()
        lax.fori_loop(first, last + 1, small, 0)
        lax.fori_loop(first, last + 1, along, 0)
        lax.fori_loop(first, last, across, 0)
        g = len(GROUPS) - 1
        arrive(h, g)
        lax.fori_loop(GROUPS[g][0], GROUPS[g][1] + 1, stage, 0)
        for r, k, row in ((first, 2, first - 1), (last, 3, last + 1)):
            small(row, 0)
            add_link(k, growth(r), r, row, PAD)
        if relayed:
            for side in range(2):
                @pl.when(me == via[side])
                def _():
                    for g in range(len(GROUPS)):
                        to_relay(side, h, g).wait_recv()
                        from_relay(side, h, g).start()
        return carry

    def out_copy(h):
        lanes = pl.ds(pl.multiple_of(h * LANES, LANES), LANES)
        return pltpu.make_async_copy(grid.at[0, h, pl.ds(first, rows), inner, :], out.at[:, :, lanes], out_sem.at[h])

    lax.fori_loop(0, halves, half, 0)

    scale = 1.0 / (m * halves * LANES)
    ours = sums[...] * jnp.exp(-temper * raw[0]) * scale
    width = cols // m
    for p in range(m):
        share[p] = ours[:, :, p * width:(p + 1) * width]

    def org_copy(d):
        peer = lax.rem(org + d, m)
        return pltpu.make_async_remote_copy(
            src_ref=share.at[peer], dst_ref=landed.at[d - 1], send_sem=org_send.at[d - 1], recv_sem=org_recv.at[d - 1],
            device_id={"org": peer}, device_id_type=MESH)
    for d in range(1, m):
        org_copy(d).start()
    final = share[org]
    for d in range(1, m):
        org_copy(d).wait_recv()
        final += landed[d - 1]
    weights[...] = final

    for d in range(1, m):
        org_copy(d).wait_send()
    for h in range(halves):
        out_copy(h).wait()
    for side in range(2):
        @pl.when(sides[side][0])
        def _():
            cost_copy(side).wait_send()
    for h in range(halves):
        for g in range(len(GROUPS)):
            each_send(h, g, lambda copy: copy.wait_send())
            if relayed:
                for side in range(2):
                    @pl.when(me == via[side])
                    def _():
                        from_relay(side, h, g).wait_send()


def local(n, m, warm_labels, link_costs, anchor_nodes, demand):
    rows, cols, count = warm_labels.shape
    halves = count // LANES
    total = rows + 2 * HALO
    width = cols // m
    any_space = pl.BlockSpec(memory_space=pl.ANY)
    vmem = pl.BlockSpec(memory_space=pltpu.VMEM)
    dma = pltpu.SemaphoreType.DMA
    return pl.pallas_call(
        functools.partial(kernel, n, m, rows, cols, halves),
        out_shape=(
            jax.ShapeDtypeStruct((rows, cols, count), jnp.float32),
            jax.ShapeDtypeStruct((4, rows, width), jnp.float32),
        ),
        in_specs=[any_space, any_space, vmem, vmem],
        out_specs=(any_space, vmem),
        scratch_shapes=[
            pltpu.VMEM((2, halves, total, cols + 2 * PAD, LANES), jnp.float32),
            pltpu.VMEM((4, total, cols, LANES), jnp.float32),
            pltpu.VMEM((4, 4, rows, cols), jnp.float32),
            pltpu.VMEM((cols, 16 * rows), jnp.float32),
            pltpu.VMEM((4, rows, cols), jnp.float32),
            pltpu.VMEM((m, 4, rows, width), jnp.float32),
            pltpu.VMEM((max(m - 1, 1), 4, rows, width), jnp.float32),
            pltpu.VMEM((halves, HALO, cols - cols // 2, LANES), jnp.float32),
            pltpu.VMEM((rows + 2, cols + 2 * PAD, LANES), jnp.float32),
            dma((2, halves, len(GROUPS), 2)),
            dma((2, halves, len(GROUPS), 2)),
            dma((halves, len(GROUPS))),
            dma((halves, len(GROUPS))),
            dma((2,)),
            dma((2,)),
            dma((max(m - 1, 1),)),
            dma((max(m - 1, 1),)),
            dma((halves + 1,)),
            dma((halves,)),
        ],
        compiler_params=pltpu.CompilerParams(collective_id=0, has_side_effects=True, vmem_limit_bytes=60 * 1024 * 1024),
    )(warm_labels, link_costs, anchor_nodes.reshape(halves, 1, LANES), demand.reshape(halves, 1, LANES))


def solution(mesh):
    placed = (P("blk", None, "org"), P(None, "blk", None), P("org"), P("org"))
    return jax.shard_map(
        functools.partial(local, mesh.shape["blk"], mesh.shape["org"]),
        mesh=mesh,
        in_specs=placed,
        out_specs=(P("blk", None, "org"), P(None, "blk", "org")),
        check_vma=False,
    )
```

```python
import functools

import jax
import jax.numpy as jnp
from jax import lax
from jax.experimental import pallas as pl
from jax.experimental.pallas import tpu as pltpu
from jax.sharding import PartitionSpec as P

INNER = 2
ROUNDS = 3
STEPS = INNER * ROUNDS
HALO = STEPS + 1

far_value = 1000000000.0
temper = 0.5
LANES = 128
PAD = 8
CHUNK = 64
MESH = pl.DeviceIdType.MESH
GROUPS = ((1, HALO - 3), (HALO - 2, HALO - 1), (HALO, HALO))


def kernel(n, m, rows, cols, halves, warm, costs, anchors, demand, out, weights, grid, wide, raw, turned, sums, share,
           landed, relay, decay, row_send, row_recv, relay_in, relay_out, cost_send, cost_recv, org_send, org_recv, local_sem, out_sem):
    me = lax.axis_index("blk")
    org = lax.axis_index("org")
    has_top = me > 0
    has_bottom = me < n - 1
    top = {"blk": jnp.maximum(me - 1, 0)}
    bottom = {"blk": jnp.minimum(me + 1, n - 1)}
    first, last = HALO, HALO + rows - 1
    inner = pl.ds(PAD, cols)
    sides = ((has_top, top), (has_bottom, bottom))
    mid = n // 2
    relayed = n == 8
    via = (0, n - 1)
    goal = (mid - 1, mid)
    splits = tuple(relayed and me == goal[1 - side] for side in range(2))
    cut = cols // 2

    barrier = pltpu.get_barrier_semaphore()
    for there, who in sides:
        @pl.when(there)
        def _():
            pl.semaphore_signal(barrier, inc=1, device_id=who, device_id_type=MESH)
    for d in range(1, m):
        pl.semaphore_signal(barrier, inc=1, device_id={"org": lax.rem(org + d, m)}, device_id_type=MESH)
    if relayed:
        for a, b in ((mid - 1, 0), (mid - 1, n - 1), (mid, 0), (mid, n - 1)):
            for mine, other in ((a, b), (b, a)):
                @pl.when(me == mine)
                def _():
                    pl.semaphore_signal(barrier, inc=1, device_id={"blk": other}, device_id_type=MESH)
    own_cost = pltpu.make_async_copy(costs, raw.at[0], local_sem.at[halves])
    own_cost.start()

    def own_rows(h):
        return pltpu.make_async_copy(
            warm.at[:, :, pl.ds(h * LANES, LANES)],
            grid.at[0, h, pl.ds(first, rows), inner, :],
            local_sem.at[h])
    for h in range(halves):
        own_rows(h).start()
    pl.semaphore_wait(barrier, m - 1 + jnp.where(has_top, 1, 0) + jnp.where(has_bottom, 1, 0)
                      + (jnp.where((me == 0) | (me == n - 1) | (me == mid) | (me == mid - 1), 2, 0) if relayed else 0))

    def cost_copy(side):
        return pltpu.make_async_remote_copy(
            src_ref=costs, dst_ref=raw.at[2 - side], send_sem=cost_send.at[side], recv_sem=cost_recv.at[side],
            device_id=sides[side][1], device_id_type=MESH)

    def ranges(side, g):
        low, high = GROUPS[g]
        count = high - low + 1
        if side == 0:
            return pl.ds(low - 1, count), pl.ds(last + low, count), pl.ds(low - 1, count)
        return pl.ds(rows - high, count), pl.ds(first - high, count), pl.ds(first - high, count)

    def lane_range(h):
        return pl.ds(pl.multiple_of(h * LANES, LANES), LANES)

    def row_copy(side, h, g, width):
        source, target, _ = ranges(side, g)
        return pltpu.make_async_remote_copy(
            src_ref=warm.at[source, pl.ds(0, width), lane_range(h)],
            dst_ref=grid.at[0, h, target, pl.ds(PAD, width), :],
            send_sem=row_send.at[side, h, g, 0], recv_sem=row_recv.at[side, h, g, 0],
            device_id=sides[side][1], device_id_type=MESH)

    def to_relay(side, h, g):
        source, _, slots = ranges(side, g)
        return pltpu.make_async_remote_copy(
            src_ref=warm.at[source, pl.ds(cut, cols - cut), lane_range(h)],
            dst_ref=relay.at[h, slots],
            send_sem=row_send.at[side, h, g, 1], recv_sem=relay_in.at[h, g],
            device_id={"blk": via[side]}, device_id_type=MESH)

    def from_relay(side, h, g):
        _, target, slots = ranges(side, g)
        return pltpu.make_async_remote_copy(
            src_ref=relay.at[h, slots],
            dst_ref=grid.at[0, h, target, pl.ds(PAD + cut, cols - cut), :],
            send_sem=relay_out.at[h, g], recv_sem=row_recv.at[side, h, g, 1],
            device_id={"blk": goal[side]}, device_id_type=MESH)

    def each_send(h, g, act):
        for side in range(2):
            there, split = sides[side][0], splits[side]
            @pl.when(there & jnp.logical_not(split) if relayed else there)
            def _():
                act(row_copy(side, h, g, cols))
            if relayed:
                @pl.when(split)
                def _():
                    act(to_relay(side, h, g))
                    act(row_copy(side, h, g, cut))

    def arrive(h, g):
        for side in range(2):
            there, split = sides[1 - side][0], splits[1 - side]
            @pl.when(there & jnp.logical_not(split) if relayed else there)
            def _():
                row_copy(side, h, g, cols).wait_recv()
            if relayed:
                @pl.when(split)
                def _():
                    row_copy(side, h, g, cut).wait_recv()
                    from_relay(side, h, g).wait_recv()

    for side in range(2):
        @pl.when(sides[side][0])
        def _():
            cost_copy(side).start()
    for h in range(halves):
        for g in range(len(GROUPS)):
            each_send(h, g, lambda copy: copy.start())

    edge = jnp.full((PAD, LANES), far_value, jnp.float32)
    total = rows + 2 * HALO

    def fill_edges(r, carry):
        for b in range(2):
            for h in range(halves):
                grid[b, h, r, pl.ds(0, PAD), :] = edge
                grid[b, h, r, pl.ds(PAD + cols, PAD), :] = edge
        return carry
    lax.fori_loop(0, total, fill_edges, 0)
    raw[3] = jnp.zeros_like(raw[3])
    for missing, block, begin in ((me == 0, 1, 0), (me == n - 1, 2, last + 1)):
        @pl.when(missing)
        def _():
            raw[block] = jnp.full(raw.shape[1:], far_value, jnp.float32)
            def fill(r, carry):
                for h in range(halves):
                    grid[0, h, begin + r, inner, :] = jnp.full((cols, LANES), far_value, jnp.float32)
                return carry
            lax.fori_loop(0, HALO, fill, 0)

    own_cost.wait()
    for side in range(2):
        @pl.when(sides[1 - side][0])
        def _():
            cost_copy(side).wait_recv()
    turned[...] = jnp.transpose(raw[...].reshape(4 * 4 * rows, cols))

    def widen(i, carry):
        piece = turned[pl.ds(pl.multiple_of(i * 8, 8), 8), :]
        for r in range(1, total - 1):
            if r < first:
                block, row = 1, rows - first + r
            elif r <= last:
                block, row = 0, r - first
            else:
                block, row = 2, r - last - 1
            for k in range(4):
                lane = (block * 4 + k) * rows + row
                wide[k, r, pl.ds(pl.multiple_of(i * 8, 8), 8), :] = jnp.broadcast_to(piece[:, lane:lane + 1], (8, LANES))
        return carry
    lax.fori_loop(0, cols // 8, widen, 0)

    def place(h, r):
        names = anchors[h]
        base = (me * rows + r - first) * cols
        for i in range(cols // CHUNK):
            node = lax.broadcasted_iota(jnp.int32, (CHUNK, LANES), 0) + (base + i * CHUNK)
            at = pl.ds(PAD + i * CHUNK, CHUNK)
            grid[0, h, r, at, :] = jnp.where(node == names, 0.0, grid[0, h, r, at, :])

    def relax(h, r, s):
        old, new = lax.rem(s + 1, 2), lax.rem(s, 2)
        for i in range(cols // CHUNK):
            c0 = PAD + i * CHUNK
            at, cut = pl.ds(c0, CHUNK), pl.ds(i * CHUNK, CHUNK)
            best = grid[old, h, r, at, :]
            best = jnp.minimum(best, grid[old, h, r, pl.ds(c0 - 1, CHUNK), :] + wide[0, r, cut, :])
            best = jnp.minimum(best, grid[old, h, r, pl.ds(c0 + 1, CHUNK), :] + wide[1, r, cut, :])
            best = jnp.minimum(best, grid[old, h, r - 1, at, :] + wide[2, r, cut, :])
            best = jnp.minimum(best, grid[old, h, r + 1, at, :] + wide[3, r, cut, :])
            grid[new, h, r, at, :] = best

    ones = jnp.ones((8, 2 * LANES), jnp.bfloat16)
    sums[...] = jnp.zeros_like(sums)
    middle = rows // 2
    zero_edge = jnp.zeros((PAD, LANES), jnp.float32)
    for r in range(rows + 2):
        decay[r, pl.ds(0, PAD), :] = zero_edge
        decay[r, pl.ds(PAD + cols, PAD), :] = zero_edge

    def begin(h, carry):
        own_rows(h).wait()

        def place_own(r, carry):
            place(h, r)
            return carry
        lax.fori_loop(first, last + 1, place_own, 0)
        for s in range(1, middle):
            def inside(r, carry):
                relax(h, r, jnp.int32(s))
                return carry
            lax.fori_loop(first + s, last - s + 1, inside, 0)
        return carry
    lax.fori_loop(0, halves, begin, 0)

    def half(h, carry):
        if relayed:
            for side in range(2):
                @pl.when(me == via[side])
                def _():
                    for g in range(len(GROUPS)):
                        to_relay(side, h, g).wait_recv()
                        from_relay(side, h, g).start()

        def stage(j, carry):
            place(h, first - j)
            place(h, last + j)

            def diagonal(s, carry):
                relax(h, first - j + s, s)
                relax(h, last + j - s, s)
                return carry
            return lax.fori_loop(1, jnp.minimum(STEPS, j + middle - 1) + 1, diagonal, carry)

        def small(r, carry):
            for i in range(cols // CHUNK):
                at = pl.ds(PAD + i * CHUNK, CHUNK)
                decay[r - first + 1, at, :] = jnp.exp(-temper * grid[0, h, r, at, :])
            return carry

        def add_link(k, own, r, row, start):
            term = own * decay[row - first + 1, pl.ds(start, cols), :]
            high = term.astype(jnp.bfloat16)
            low = (term - high.astype(jnp.float32)).astype(jnp.bfloat16)
            part = lax.dot_general(ones, jnp.concatenate([high, low], axis=1), (((1,), (1,)), ((), ())),
                                   preferred_element_type=jnp.float32)
            sums[k, pl.ds(r - first, 1), :] += part[0:1]

        def growth(r):
            return demand[h] * jnp.exp(temper * grid[0, h, r, inner, :])

        def along(r, carry):
            own = growth(r)
            add_link(0, own, r, r, PAD - 1)
            add_link(1, own, r, r, PAD + 1)
            return carry

        def across(r, carry):
            add_link(3, growth(r), r, r + 1, PAD)
            add_link(2, growth(r + 1), r + 1, r, PAD)
            return carry

        for g in range(len(GROUPS) - 1):
            arrive(h, g)
            lax.fori_loop(GROUPS[g][0], GROUPS[g][1] + 1, stage, 0)
        out_copy(h).start()
        lax.fori_loop(first, last + 1, small, 0)
        lax.fori_loop(first, last + 1, along, 0)
        lax.fori_loop(first, last, across, 0)
        g = len(GROUPS) - 1
        arrive(h, g)
        lax.fori_loop(GROUPS[g][0], GROUPS[g][1] + 1, stage, 0)
        for r, k, row in ((first, 2, first - 1), (last, 3, last + 1)):
            small(row, 0)
            add_link(k, growth(r), r, row, PAD)
        return carry

    def out_copy(h):
        lanes = pl.ds(pl.multiple_of(h * LANES, LANES), LANES)
        return pltpu.make_async_copy(grid.at[0, h, pl.ds(first, rows), inner, :], out.at[:, :, lanes], out_sem.at[h])

    lax.fori_loop(0, halves, half, 0)

    scale = 1.0 / (m * halves * LANES)
    ours = sums[...] * jnp.exp(-temper * raw[0]) * scale
    width = cols // m
    for p in range(m):
        share[p] = ours[:, :, p * width:(p + 1) * width]

    def org_copy(d):
        peer = lax.rem(org + d, m)
        return pltpu.make_async_remote_copy(
            src_ref=share.at[peer], dst_ref=landed.at[d - 1], send_sem=org_send.at[d - 1], recv_sem=org_recv.at[d - 1],
            device_id={"org": peer}, device_id_type=MESH)
    for d in range(1, m):
        org_copy(d).start()
    final = share[org]
    for d in range(1, m):
        org_copy(d).wait_recv()
        final += landed[d - 1]
    weights[...] = final

    for d in range(1, m):
        org_copy(d).wait_send()
    for h in range(halves):
        out_copy(h).wait()
    for side in range(2):
        @pl.when(sides[side][0])
        def _():
            cost_copy(side).wait_send()
    for h in range(halves):
        for g in range(len(GROUPS)):
            each_send(h, g, lambda copy: copy.wait_send())
            if relayed:
                for side in range(2):
                    @pl.when(me == via[side])
                    def _():
                        from_relay(side, h, g).wait_send()


def local(n, m, warm_labels, link_costs, anchor_nodes, demand):
    rows, cols, count = warm_labels.shape
    halves = count // LANES
    total = rows + 2 * HALO
    width = cols // m
    any_space = pl.BlockSpec(memory_space=pl.ANY)
    vmem = pl.BlockSpec(memory_space=pltpu.VMEM)
    dma = pltpu.SemaphoreType.DMA
    return pl.pallas_call(
        functools.partial(kernel, n, m, rows, cols, halves),
        out_shape=(
            jax.ShapeDtypeStruct((rows, cols, count), jnp.float32),
            jax.ShapeDtypeStruct((4, rows, width), jnp.float32),
        ),
        in_specs=[any_space, any_space, vmem, vmem],
        out_specs=(any_space, vmem),
        scratch_shapes=[
            pltpu.VMEM((2, halves, total, cols + 2 * PAD, LANES), jnp.float32),
            pltpu.VMEM((4, total, cols, LANES), jnp.float32),
            pltpu.VMEM((4, 4, rows, cols), jnp.float32),
            pltpu.VMEM((cols, 16 * rows), jnp.float32),
            pltpu.VMEM((4, rows, cols), jnp.float32),
            pltpu.VMEM((m, 4, rows, width), jnp.float32),
            pltpu.VMEM((max(m - 1, 1), 4, rows, width), jnp.float32),
            pltpu.VMEM((halves, HALO, cols - cols // 2, LANES), jnp.float32),
            pltpu.VMEM((rows + 2, cols + 2 * PAD, LANES), jnp.float32),
            dma((2, halves, len(GROUPS), 2)),
            dma((2, halves, len(GROUPS), 2)),
            dma((halves, len(GROUPS))),
            dma((halves, len(GROUPS))),
            dma((2,)),
            dma((2,)),
            dma((max(m - 1, 1),)),
            dma((max(m - 1, 1),)),
            dma((halves + 1,)),
            dma((halves,)),
        ],
        compiler_params=pltpu.CompilerParams(collective_id=0, has_side_effects=True, vmem_limit_bytes=60 * 1024 * 1024),
    )(warm_labels, link_costs, anchor_nodes.reshape(halves, 1, LANES), demand.reshape(halves, 1, LANES))


def solution(mesh):
    placed = (P("blk", None, "org"), P(None, "blk", None), P("org"), P("org"))
    return jax.shard_map(
        functools.partial(local, mesh.shape["blk"], mesh.shape["org"]),
        mesh=mesh,
        in_specs=placed,
        out_specs=(P("blk", None, "org"), P(None, "blk", "org")),
        check_vma=False,
    )
```
